32 devices in a mesh: gp: 2 (over x), blk: 16 (over z, y, core).
Axes of the slice: x: 2, y: 2, z: 4, core: 2. Of those that a mesh axis runs over, the one named last changes fastest.
Arguments:
- points: float32 [8, 8192], P(None, ('gp', 'blk')), parts along dimension 1, may hold values from -6 to 6
- vectors: float32 [8, 8192], P(None, ('gp', 'blk')), parts along dimension 1, may hold values from -6 to 6
- inv_length: float32 [16], P('gp'), parts along dimension 0, may hold values from 0.15 to 0.6
- noise: float32 [2], P('gp'), parts along dimension 0, may hold values from 0.1 to 1
Outputs:
- product: float32 [8, 8192], P(None, ('gp', 'blk')), parts along dimension 1
The draws below stay inside these ranges and needn't reach their ends.
There are 2 independent parts, one for each index of `gp`. The reference program is written for one: setup_inputs(seed, part) draws one part's arguments, and reference() takes and returns one part's arrays. A program takes and returns all parts, laid end to end along the dimension named above; each array names one. Nothing has to cross between parts.
All inputs are finite; a program needn't handle non-finite values.
Results may differ from the reference program's by a relative error of at most 0.00017.
Values sent between devices are 32-bit elements; how exact they have to be, the bound alone decides.
No kernel may reach another device: no remote copies, remote signals or barrier semaphores. Data moves between devices by JAX's collectives and lax.ppermute only.
A program may use at most 64 MiB of HBM per device.

```python
import math
import jax
import jax.numpy as jnp
from jax import lax

DIM = 8
RHS = 8
PTS_DEV = 256
NPTS = 4096


def block_levels(stream_key, extent, pieces, low, high):
    factor_of, own = 1.0, jax.random.fold_in(stream_key, 6)
    for position, shards_of in pieces:
        draws = jnp.exp(jax.random.uniform(jax.random.fold_in(own, position), (shards_of,), jnp.float32, low / len(pieces), high / len(pieces)))
        factor_of = factor_of * jnp.repeat(draws, extent[position] // shards_of).reshape([-1 if axis == position else 1 for axis in range(len(extent))])
    return factor_of


def centred(key, extent, spread, bound, shards=(), kind=jnp.bfloat16):
    loudness = block_levels(key, extent, shards, -0.22, 0.18) if shards else 1.0
    values = jax.random.normal(key, extent, jnp.float32) * spread * loudness
    return jnp.minimum(jnp.maximum(values, -bound), bound).astype(kind)


def setup_inputs(seed: int = 0, part: int = 0) -> dict:
    key_list = jax.random.split(jax.random.key(seed), 5)
    own_keys = jax.random.split(jax.random.fold_in(key_list[4], part), 5)
    points = centred(own_keys[0], (DIM, NPTS), 1.0, 6.0, ((1, 16),), jnp.float32)
    vectors = centred(own_keys[1], (RHS, NPTS), 1.0, 6.0, ((1, 16),), jnp.float32)
    inv_length = jnp.clip(jnp.exp(jax.random.uniform(own_keys[2], (DIM,), jnp.float32, math.log(0.15), math.log(0.6))), 0.15, 0.6)
    noise = jnp.clip(jnp.exp(jax.random.uniform(own_keys[3], (1,), jnp.float32, math.log(0.1), math.log(1.0))), 0.1, 1.0)
    return {"points": points, "vectors": vectors, "inv_length": inv_length, "noise": noise}


def matern(left, right, inv_length):
    scaled_left = left * inv_length[:, None]
    scaled_right = right * inv_length[:, None]
    sq_left = lax.optimization_barrier(jnp.sum(scaled_left * scaled_left, axis=0))
    sq_right = lax.optimization_barrier(jnp.sum(scaled_right * scaled_right, axis=0))
    cross = jnp.dot(scaled_left.T, scaled_right, precision=lax.Precision.HIGHEST, preferred_element_type=jnp.float32)
    dist2 = jnp.maximum(sq_left[:, None] + sq_right[None, :] - 2.0 * cross, 0.0)
    scaled_dist = jnp.sqrt(5.0 * dist2)
    return (1.0 + scaled_dist + scaled_dist * scaled_dist / 3.0) * jnp.exp(-scaled_dist)

def reference(points, vectors, inv_length, noise):
    blocks = points.reshape(DIM, NPTS // PTS_DEV, PTS_DEV).transpose(1, 0, 2)

    def one_block(block):
        tile = matern(points, block, inv_length)
        return jnp.dot(vectors, tile, precision=lax.Precision.HIGHEST, preferred_element_type=jnp.float32)
    sums = lax.map(one_block, blocks)
    sums = sums.transpose(1, 0, 2).reshape(RHS, NPTS)
    return noise[0] * vectors + sums / jnp.sqrt(jnp.float32(NPTS))
```

```python
import functools
import math

import jax
import jax.numpy as jnp
from jax import lax
from jax.experimental import pallas as pl
from jax.experimental.pallas import tpu as pltpu
from jax.sharding import PartitionSpec as P


F32, BF16 = jnp.float32, jnp.bfloat16
LOG2E = math.log2(math.e)
SUBLANES = 8
VMEM = pl.BlockSpec(memory_space=pltpu.VMEM)
SMEM = pl.BlockSpec(memory_space=pltpu.SMEM)
PARAMS = pltpu.CompilerParams(vmem_limit_bytes=8 * 2**20)


def split3(value):
    high = value.astype(BF16).astype(F32)
    rest = value - high
    middle = rest.astype(BF16).astype(F32)
    return high, middle, rest - middle


def norm_rows(value, norms_first):
    norm = jnp.sum(value * value, axis=0, keepdims=True)
    row = lax.broadcasted_iota(jnp.int32, (SUBLANES, value.shape[1]), 0)
    start = 0 if norms_first else 3
    rows = jnp.where(row < 6, 1.0, 0.0)
    for offset, addend in enumerate(split3(norm)):
        rows = jnp.where(row == start + offset, addend, rows)
    return rows


def stack(pieces):
    pieces = list(pieces)
    if sum(p.shape[0] for p in pieces) % (2 * SUBLANES):
        pieces.append(jnp.zeros_like(pieces[-1]))
    return jnp.concatenate(pieces, axis=0).astype(BF16)


def other_side(value):
    high, middle, low = split3(value)
    return stack([high, high, middle, middle, high, low, norm_rows(value, True)])


def own_side(value):
    high, middle, low = (-2.0 * part for part in split3(value))
    return stack([high, middle, high, middle, low, high, norm_rows(value, False)])


def three_kernel(scaled_dist2):
    scaled_dist2 = jnp.maximum(scaled_dist2, 1e-30)
    dist = scaled_dist2 * lax.rsqrt(scaled_dist2)
    shifted = dist + 1.5
    return (shifted * shifted + 0.75) * jnp.exp2(dist * -LOG2E)


def block_sum(dim, block, scale, own):
    points, vectors = block[:dim] * scale, block[dim:]
    dist2 = lax.dot_general(
        other_side(points), own, (((0,), (0,)), ((), ())), preferred_element_type=F32
    )
    tile = three_kernel(dist2)
    tile_high = tile.astype(BF16)
    tile_low = (tile - tile_high.astype(F32)).astype(BF16)
    vec_high = vectors.astype(BF16)
    vec = jnp.concatenate([vec_high, (vectors - vec_high.astype(F32)).astype(BF16)], axis=0)
    both = jnp.dot(vec, tile_high, preferred_element_type=F32) + jnp.dot(
        vec, tile_low, preferred_element_type=F32
    )
    return both[: vectors.shape[0]] + both[vectors.shape[0] :]


def prepare(dim, own_ref, inv_ref, noise_ref, scale_ref, side_ref, base_ref):
    row = lax.broadcasted_iota(jnp.int32, (dim, own_ref.shape[1]), 0)
    inv = jnp.zeros(row.shape, F32)
    for d in range(dim):
        inv = jnp.where(row == d, inv_ref[d], inv)
    scale = inv * math.sqrt(5.0)
    scale_ref[...] = scale
    side_ref[...] = own_side(own_ref[:dim] * scale)
    base_ref[...] = own_ref[dim:] * noise_ref[0]


def add_blocks(dim, rows, factor, blocks_ref, scale_ref, side_ref, acc_ref, *rest):
    base_ref, out_ref = rest if len(rest) == 2 else (None, rest[0])
    count = blocks_ref.shape[0] // rows
    group = math.gcd(count, 4)
    scale, own = scale_ref[...], side_ref[...]

    def step(index, total):
        for k in range(group):
            start = pl.multiple_of((index * group + k) * rows, rows)
            total = total + block_sum(dim, blocks_ref[pl.ds(start, rows)], scale, own)
        return total

    if count == group:
        total = step(0, acc_ref[...])
    else:
        total = lax.fori_loop(0, count // group, step, acc_ref[...])
    out_ref[...] = total if base_ref is None else base_ref[...] + total * factor


def cost(rows, blocks, width):
    tile = blocks // rows * width * width
    return pl.CostEstimate(flops=tile * 400, bytes_accessed=4 * blocks * width, transcendentals=2 * tile)


def on_device(points, vectors, inv_length, noise):
    count = lax.axis_size("blk")
    dim, width = points.shape
    rhs = vectors.shape[0]
    rows = dim + rhs
    small = jax.ShapeDtypeStruct((rhs, width), F32)
    own = jnp.concatenate([points, vectors], axis=0)

    def swap(value, mask):
        return lax.ppermute(value, "blk", [(i, i ^ mask) for i in range(count)])

    levels = count.bit_length() - 1
    if count != 1 << levels or levels < 2:
        pieces = [lax.all_gather(own, "blk", axis=0, tiled=True)]
    else:
        held = own
        for bit in range(levels - 1, 1, -1):
            held = jnp.concatenate([held, swap(held, 1 << bit | 1)], axis=0)
        far = swap(held, 3)
        pieces = [held, swap(held, 1), far, swap(far, 1)]

    side_rows = -(-(6 * dim + SUBLANES) // (2 * SUBLANES)) * 2 * SUBLANES
    prepare_call = pl.pallas_call(
        functools.partial(prepare, dim),
        out_shape=[
            jax.ShapeDtypeStruct((dim, width), F32),
            jax.ShapeDtypeStruct((side_rows, width), BF16),
            small,
        ],
        in_specs=[VMEM, SMEM, SMEM],
        out_specs=[VMEM] * 3,
        name="prepare",
        compiler_params=PARAMS,
        cost_estimate=pl.CostEstimate(flops=100000, bytes_accessed=4 * rows * width, transcendentals=0),
    )
    scale, side, base = prepare_call(own, inv_length, noise)

    factor = 1.0 / (3.0 * math.sqrt(width * count))
    total = jnp.zeros((rhs, width), F32)
    for index, piece in enumerate(pieces):
        last = index == len(pieces) - 1
        add_call = pl.pallas_call(
            functools.partial(add_blocks, dim, rows, factor),
            out_shape=small,
            in_specs=[VMEM] * (5 if last else 4),
            out_specs=VMEM,
            compiler_params=PARAMS,
            cost_estimate=cost(rows, piece.shape[0], width),
        )
        total = add_call(piece, scale, side, total, *([base] if last else []))
    return total


def solution(mesh):
    return jax.shard_map(
        on_device,
        mesh=mesh,
        in_specs=(P(None, ("gp", "blk")), P(None, ("gp", "blk")), P("gp"), P("gp")),
        out_specs=P(None, ("gp", "blk")),
        check_vma=False,
    )
```

```python
import functools
import math

import jax
import jax.numpy as jnp
from jax import lax
from jax.experimental import pallas as pl
from jax.experimental.pallas import tpu as pltpu
from jax.sharding import PartitionSpec as P


F32, BF16 = jnp.float32, jnp.bfloat16
LOG2E = math.log2(math.e)
SUBLANES = 8
VMEM = pl.BlockSpec(memory_space=pltpu.VMEM)
SMEM = pl.BlockSpec(memory_space=pltpu.SMEM)
PARAMS = pltpu.CompilerParams(vmem_limit_bytes=8 * 2**20)


def split3(value):
    high = value.astype(BF16).astype(F32)
    rest = value - high
    middle = rest.astype(BF16).astype(F32)
    return high, middle, rest - middle


def norm_rows(value, norms_first):
    norm = jnp.sum(value * value, axis=0, keepdims=True)
    row = lax.broadcasted_iota(jnp.int32, (SUBLANES, value.shape[1]), 0)
    start = 0 if norms_first else 3
    rows = jnp.where(row < 6, 1.0, 0.0)
    for offset, addend in enumerate(split3(norm)):
        rows = jnp.where(row == start + offset, addend, rows)
    return rows


def stack(pieces):
    pieces = list(pieces)
    if sum(p.shape[0] for p in pieces) % (2 * SUBLANES):
        pieces.append(jnp.zeros_like(pieces[-1]))
    return jnp.concatenate(pieces, axis=0).astype(BF16)


def other_side(value):
    high, middle, low = split3(value)
    return stack([high, high, middle, middle, high, low, norm_rows(value, True)])


def own_side(value):
    high, middle, low = (-2.0 * part for part in split3(value))
    return stack([high, middle, high, middle, low, high, norm_rows(value, False)])


def three_kernel(scaled_dist2):
    scaled_dist2 = jnp.maximum(scaled_dist2, 1e-30)
    dist = scaled_dist2 * lax.rsqrt(scaled_dist2)
    shifted = dist + 1.5
    return (shifted * shifted + 0.75) * jnp.exp2(dist * -LOG2E)


def block_sum(dim, block, scale, own):
    points, vectors = block[:dim] * scale, block[dim:]
    dist2 = lax.dot_general(
        other_side(points), own, (((0,), (0,)), ((), ())), preferred_element_type=F32
    )
    tile = three_kernel(dist2)
    tile_high = tile.astype(BF16)
    tile_low = (tile - tile_high.astype(F32)).astype(BF16)
    vec_high = vectors.astype(BF16)
    vec = jnp.concatenate([vec_high, (vectors - vec_high.astype(F32)).astype(BF16)], axis=0)
    both = jnp.dot(vec, tile_high, preferred_element_type=F32) + jnp.dot(
        vec, tile_low, preferred_element_type=F32
    )
    return both[: vectors.shape[0]] + both[vectors.shape[0] :]


def prepare(dim, own_ref, inv_ref, noise_ref, scale_ref, side_ref, base_ref):
    row = lax.broadcasted_iota(jnp.int32, (dim, own_ref.shape[1]), 0)
    inv = jnp.zeros(row.shape, F32)
    for d in range(dim):
        inv = jnp.where(row == d, inv_ref[d], inv)
    scale = inv * math.sqrt(5.0)
    scale_ref[...] = scale
    side_ref[...] = own_side(own_ref[:dim] * scale)
    base_ref[...] = own_ref[dim:] * noise_ref[0]


def add_pieces(dim, rows, factor, scale_ref, side_ref, acc_ref, *rest):
    *rest, out_ref = rest
    base_ref = rest.pop(0) if factor else None
    scale, own = scale_ref[...], side_ref[...]
    total = acc_ref[...]
    for piece_ref in rest:
        count = piece_ref.shape[0] // rows
        group = math.gcd(count, 4)

        def step(index, total, piece_ref=piece_ref, group=group):
            for k in range(group):
                start = pl.multiple_of((index * group + k) * rows, rows)
                total = total + block_sum(dim, piece_ref[pl.ds(start, rows)], scale, own)
            return total

        if count == group:
            total = step(0, total)
        else:
            total = lax.fori_loop(0, count // group, step, total)
    out_ref[...] = base_ref[...] + total * factor if factor else total


def on_device(points, vectors, inv_length, noise):
    count = lax.axis_size("blk")
    dim, width = points.shape
    rhs = vectors.shape[0]
    rows = dim + rhs
    small = jax.ShapeDtypeStruct((rhs, width), F32)
    own = jnp.concatenate([points, vectors], axis=0)

    def swap(value, mask):
        return lax.ppermute(value, "blk", [(i, i ^ mask) for i in range(count)])

    levels = count.bit_length() - 1
    if count != 1 << levels or levels < 3:
        groups = [[lax.all_gather(own, "blk", axis=0, tiled=True)]]
    else:
        held = own
        for bit in range(levels - 1, 2, -1):
            held = jnp.concatenate([held, swap(held, 1 << bit | 1)], axis=0)
        newest = swap(held, 5)
        early = swap(held, 3)
        late = swap(newest, 3)
        near = swap(jnp.concatenate([held, newest], axis=0), 1)
        early_core = swap(early, 1)
        late_core = swap(late, 1)
        groups = [[held, newest], [near], [early, early_core, late], [late_core]]

    side_rows = -(-(6 * dim + SUBLANES) // (2 * SUBLANES)) * 2 * SUBLANES
    prepare_call = pl.pallas_call(
        functools.partial(prepare, dim),
        out_shape=[
            jax.ShapeDtypeStruct((dim, width), F32),
            jax.ShapeDtypeStruct((side_rows, width), BF16),
            small,
        ],
        in_specs=[VMEM, SMEM, SMEM],
        out_specs=[VMEM] * 3,
        name="prepare",
        compiler_params=PARAMS,
        cost_estimate=pl.CostEstimate(flops=100000, bytes_accessed=4 * rows * width, transcendentals=0),
    )
    scale, side, base = prepare_call(own, inv_length, noise)

    factor = 1.0 / (3.0 * math.sqrt(width * count))
    total = jnp.zeros((rhs, width), F32)
    for index, pieces in enumerate(groups):
        last = index == len(groups) - 1
        operands = [scale, side, total] + ([base] if last else []) + pieces
        blocks = sum(piece.shape[0] for piece in pieces) // rows
        add_call = pl.pallas_call(
            functools.partial(add_pieces, dim, rows, factor if last else None),
            out_shape=small,
            in_specs=[VMEM] * len(operands),
            out_specs=VMEM,
            compiler_params=PARAMS,
            cost_estimate=pl.CostEstimate(
                flops=blocks * width * width * 400,
                bytes_accessed=4 * blocks * rows * width,
                transcendentals=2 * blocks * width * width,
            ),
        )
        total = add_call(*operands)
    return total


def solution(mesh):
    return jax.shard_map(
        on_device,
        mesh=mesh,
        in_specs=(P(None, ("gp", "blk")), P(None, ("gp", "blk")), P("gp"), P("gp")),
        out_specs=P(None, ("gp", "blk")),
        check_vma=False,
    )
```

```python
import functools
import math

import jax
import jax.numpy as jnp
from jax import lax
from jax.experimental import pallas as pl
from jax.experimental.pallas import tpu as pltpu
from jax.sharding import PartitionSpec as P


F32, BF16 = jnp.float32, jnp.bfloat16
LOG2E = math.log2(math.e)
SUBLANES = 8
VMEM = pl.BlockSpec(memory_space=pltpu.VMEM)
PARAMS = pltpu.CompilerParams(vmem_limit_bytes=8 * 2**20)


def split3(value):
    high = value.astype(BF16).astype(F32)
    rest = value - high
    middle = rest.astype(BF16).astype(F32)
    return high, middle, rest - middle


def norm_rows(value, norms_first):
    norm = jnp.sum(value * value, axis=0, keepdims=True)
    row = lax.broadcasted_iota(jnp.int32, (SUBLANES, value.shape[1]), 0)
    start = 0 if norms_first else 3
    rows = jnp.where(row < 6, 1.0, 0.0)
    for offset, addend in enumerate(split3(norm)):
        rows = jnp.where(row == start + offset, addend, rows)
    return rows


def stack(pieces):
    pieces = list(pieces)
    if sum(p.shape[0] for p in pieces) % (2 * SUBLANES):
        pieces.append(jnp.zeros_like(pieces[-1]))
    return jnp.concatenate(pieces, axis=0).astype(BF16)


def other_side(value):
    high, middle, low = split3(value)
    return stack([high, high, middle, middle, high, low, norm_rows(value, True)])


def own_side(value):
    high, middle, low = (-2.0 * part for part in split3(value))
    return stack([high, middle, high, middle, low, high, norm_rows(value, False)])


def third_kernel(value):
    value = jnp.maximum(value, 1e-30)
    third = value * lax.rsqrt(value)
    return (value + third + 1.0 / 3.0) * jnp.exp2(third * (-3.0 * LOG2E))


def block_sum(dim, block, scale, own):
    points, vectors = block[:dim] * scale, block[dim:]
    width = block.shape[1]
    other = other_side(points)
    vec_high = vectors.astype(BF16)
    vec = jnp.concatenate([vec_high, (vectors - vec_high.astype(F32)).astype(BF16)], axis=0)
    part = width // 2 if width % 256 == 0 else width
    both = 0.0
    for start in range(0, width, part):
        here = slice(start, start + part)
        value = lax.dot_general(
            other[:, here], own, (((0,), (0,)), ((), ())), preferred_element_type=F32
        )
        tile = third_kernel(value)
        high = tile.astype(BF16)
        low = (tile - high.astype(F32)).astype(BF16)
        both += jnp.dot(
            jnp.concatenate([vec[:, here]] * 2, axis=1),
            jnp.concatenate([high, low], axis=0),
            preferred_element_type=F32,
        )
    return both[: vectors.shape[0]] + both[vectors.shape[0] :]


def prepare(dim, own_ref, params_ref, scale_ref, side_ref, base_ref, sum_ref):
    here = lax.broadcasted_iota(jnp.int32, (dim, dim), 0) == lax.broadcasted_iota(
        jnp.int32, (dim, dim), 1
    )
    params = params_ref[...].reshape(1, dim + 1)
    inv = jnp.sum(jnp.where(here, params[:, :dim], 0.0), axis=1, keepdims=True)
    scale = jnp.broadcast_to(inv * (math.sqrt(5.0) / 3.0), scale_ref.shape)
    side = own_side(own_ref[:dim] * scale)
    scale_ref[...] = scale
    side_ref[...] = side
    base_ref[...] = own_ref[dim:] * params[:, dim:]
    sum_ref[...] = block_sum(dim, own_ref[...], scale, side)


def add_pieces(dim, rows, factor, scale_ref, side_ref, acc_ref, *rest):
    *rest, out_ref = rest
    base_ref = rest.pop(0) if factor else None
    scale, own = scale_ref[...], side_ref[...]
    total = acc_ref[...]
    for piece_ref in rest:
        count = piece_ref.shape[0] // rows
        group = math.gcd(count, 4)

        def step(index, total, piece_ref=piece_ref, group=group):
            for k in range(group):
                start = pl.multiple_of((index * group + k) * rows, rows)
                total = total + block_sum(dim, piece_ref[pl.ds(start, rows)], scale, own)
            return total

        if count == group:
            total = step(0, total)
        else:
            total = lax.fori_loop(0, count // group, step, total)
    out_ref[...] = base_ref[...] + total * factor if factor else total


def on_device(points, vectors, inv_length, noise):
    count = lax.axis_size("blk")
    dim, width = points.shape
    rhs = vectors.shape[0]
    rows = dim + rhs
    small = jax.ShapeDtypeStruct((rhs, width), F32)
    own = lax.optimization_barrier(jnp.concatenate([points, vectors], axis=0))
    params = lax.optimization_barrier(jnp.concatenate([inv_length, noise]))

    def swap(value, mask):
        return lax.ppermute(value, "blk", [(i, i ^ mask) for i in range(count)])

    levels = count.bit_length() - 1
    if count != 1 << levels or levels < 3:
        others = [lax.ppermute(own, "blk", [(i, (i + k) % count) for i in range(count)]) for k in range(1, count)]
        groups = [others + [newest, early], [early_core, near, late], [late_core]]
    else:
        held, others = own, []
        for bit in range(levels - 1, 2, -1):
            others.append(swap(held, 1 << bit | 1))
            held = jnp.concatenate([held, others[-1]], axis=0)
        newest = swap(held, 5)
        early = swap(held, 3)
        late = swap(newest, 3)
        near = swap(jnp.concatenate([held, newest], axis=0), 1)
        early_core = swap(early, 1)
        late_core = swap(late, 1)
        groups = [others + [newest, early], [early_core, near, late], [late_core]]

    side_rows = -(-(6 * dim + SUBLANES) // (2 * SUBLANES)) * 2 * SUBLANES
    prepare_call = pl.pallas_call(
        functools.partial(prepare, dim),
        out_shape=[
            jax.ShapeDtypeStruct((dim, width), F32),
            jax.ShapeDtypeStruct((side_rows, width), BF16),
            small,
            small,
        ],
        in_specs=[VMEM] * 2,
        out_specs=[VMEM] * 4,
        name="prepare",
        compiler_params=PARAMS,
        cost_estimate=pl.CostEstimate(flops=100000, bytes_accessed=4 * rows * width, transcendentals=0),
    )
    scale, side, base, total = prepare_call(own, params)

    factor = 3.0 / math.sqrt(width * count)
    for index, pieces in enumerate(groups):
        last = index == len(groups) - 1
        operands = [scale, side, total] + ([base] if last else []) + pieces
        blocks = sum(piece.shape[0] for piece in pieces) // rows
        add_call = pl.pallas_call(
            functools.partial(add_pieces, dim, rows, factor if last else None),
            out_shape=small,
            in_specs=[VMEM] * len(operands),
            out_specs=VMEM,
            compiler_params=PARAMS,
            cost_estimate=pl.CostEstimate(
                flops=blocks * width * width * 400,
                bytes_accessed=4 * blocks * rows * width,
                transcendentals=2 * blocks * width * width,
            ),
        )
        total = add_call(*operands)
    return total


def solution(mesh):
    return jax.shard_map(
        on_device,
        mesh=mesh,
        in_specs=(P(None, ("gp", "blk")), P(None, ("gp", "blk")), P("gp"), P("gp")),
        out_specs=P(None, ("gp", "blk")),
        check_vma=False,
    )
```

```python
import functools
import math

import jax
import jax.numpy as jnp
from jax import lax
from jax.experimental import pallas as pl
from jax.experimental.pallas import tpu as pltpu
from jax.sharding import PartitionSpec as P


F32, BF16 = jnp.float32, jnp.bfloat16
LOG2E = math.log2(math.e)
SUBLANES = 8
VMEM = pl.BlockSpec(memory_space=pltpu.VMEM)
PARAMS = pltpu.CompilerParams(vmem_limit_bytes=8 * 2**20)


def split3(value):
    high = value.astype(BF16).astype(F32)
    rest = value - high
    middle = rest.astype(BF16).astype(F32)
    return high, middle, rest - middle


def norm_rows(value, norms_first):
    norm = jnp.sum(value * value, axis=0, keepdims=True)
    row = lax.broadcasted_iota(jnp.int32, (SUBLANES, value.shape[1]), 0)
    start = 0 if norms_first else 3
    rows = jnp.where(row < 6, 1.0, 0.0)
    for offset, addend in enumerate(split3(norm)):
        rows = jnp.where(row == start + offset, addend, rows)
    return rows


def stack(pieces):
    pieces = list(pieces)
    if sum(p.shape[0] for p in pieces) % (2 * SUBLANES):
        pieces.append(jnp.zeros_like(pieces[-1]))
    return jnp.concatenate(pieces, axis=0).astype(BF16)


def other_side(value):
    high, middle, low = split3(value)
    return stack([high, high, middle, middle, high, low, norm_rows(value, True)])


def own_side(value):
    high, middle, low = (-2.0 * part for part in split3(value))
    return stack([high, middle, high, middle, low, high, norm_rows(value, False)])


def third_kernel(value):
    value = jnp.maximum(value, 1e-30)
    third = value * lax.rsqrt(value)
    return (value + third + 1.0 / 3.0) * jnp.exp2(third * (-3.0 * LOG2E))


def block_sum(dim, block, scale, own):
    points, vectors = block[:dim] * scale, block[dim:]
    width = block.shape[1]
    other = other_side(points)
    vec_high = vectors.astype(BF16)
    vec = jnp.concatenate([vec_high, (vectors - vec_high.astype(F32)).astype(BF16)], axis=0)
    part = width // 2 if width % 256 == 0 else width
    both = 0.0
    for start in range(0, width, part):
        here = slice(start, start + part)
        value = lax.dot_general(
            other[:, here], own, (((0,), (0,)), ((), ())), preferred_element_type=F32
        )
        tile = third_kernel(value)
        high = tile.astype(BF16)
        low = (tile - high.astype(F32)).astype(BF16)
        both += jnp.dot(
            jnp.concatenate([vec[:, here]] * 2, axis=1),
            jnp.concatenate([high, low], axis=0),
            preferred_element_type=F32,
        )
    return both[: vectors.shape[0]] + both[vectors.shape[0] :]


def prepare(dim, own_ref, params_ref, scale_ref, side_ref, base_ref, sum_ref):
    here = lax.broadcasted_iota(jnp.int32, (dim, dim), 0) == lax.broadcasted_iota(
        jnp.int32, (dim, dim), 1
    )
    params = params_ref[...].reshape(1, dim + 1)
    inv = jnp.sum(jnp.where(here, params[:, :dim], 0.0), axis=1, keepdims=True)
    scale = jnp.broadcast_to(inv * (math.sqrt(5.0) / 3.0), scale_ref.shape)
    side = own_side(own_ref[:dim] * scale)
    scale_ref[...] = scale
    side_ref[...] = side
    base_ref[...] = own_ref[dim:] * params[:, dim:]
    sum_ref[...] = block_sum(dim, own_ref[...], scale, side)


def add_pieces(dim, rows, factor, scale_ref, side_ref, acc_ref, *rest):
    *rest, out_ref = rest
    base_ref = rest.pop(0) if factor else None
    scale, own = scale_ref[...], side_ref[...]
    total = acc_ref[...]
    for piece_ref in rest:
        count = piece_ref.shape[0] // rows
        group = count if count <= 8 else math.gcd(count, 8)

        def step(index, total, piece_ref=piece_ref, group=group):
            for k in range(group):
                start = pl.multiple_of((index * group + k) * rows, rows)
                total = total + block_sum(dim, piece_ref[pl.ds(start, rows)], scale, own)
            return total

        if count == group:
            total = step(0, total)
        else:
            total = lax.fori_loop(0, count // group, step, total)
    out_ref[...] = base_ref[...] + total * factor if factor else total


def on_device(points, vectors, inv_length, noise):
    count = lax.axis_size("blk")
    dim, width = points.shape
    rhs = vectors.shape[0]
    rows = dim + rhs
    small = jax.ShapeDtypeStruct((rhs, width), F32)
    own = lax.optimization_barrier(jnp.concatenate([points, vectors], axis=0))
    params = lax.optimization_barrier(jnp.concatenate([inv_length, noise]))

    def swap(value, masks):
        pairs = [(i, i ^ masks[(i & 7).bit_count() % 2]) for i in range(count)]
        return lax.ppermute(value, "blk", pairs)

    levels = count.bit_length() - 1
    if count != 1 << levels or levels < 3:
        others = [lax.ppermute(own, "blk", [(i, (i + k) % count) for i in range(count)]) for k in range(1, count)]
        groups = [others + [newest, early, near_held], [near, late], [late_core]]
    else:
        held, others = own, []
        for bit in range(levels - 1, 2, -1):
            others.append(swap(held, (1 << bit | 1,) * 2))
            held = jnp.concatenate([held, others[-1]], axis=0)
        newest = swap(held, (5, 3))
        early = swap(held, (3, 5))
        late = swap(newest, (3, 5))
        near_held = swap(held, (1, 1))
        near = swap(jnp.concatenate([newest, early], axis=0), (1, 1))
        late_core = swap(late, (1, 1))
        groups = [others + [newest, early, near_held], [near, late], [late_core]]

    side_rows = -(-(6 * dim + SUBLANES) // (2 * SUBLANES)) * 2 * SUBLANES
    prepare_call = pl.pallas_call(
        functools.partial(prepare, dim),
        out_shape=[
            jax.ShapeDtypeStruct((dim, width), F32),
            jax.ShapeDtypeStruct((side_rows, width), BF16),
            small,
            small,
        ],
        in_specs=[VMEM] * 2,
        out_specs=[VMEM] * 4,
        name="prepare",
        compiler_params=PARAMS,
        cost_estimate=pl.CostEstimate(flops=100000, bytes_accessed=4 * rows * width, transcendentals=0),
    )
    scale, side, base, total = prepare_call(own, params)

    factor = 3.0 / math.sqrt(width * count)
    for index, pieces in enumerate(groups):
        last = index == len(groups) - 1
        operands = [scale, side, total] + ([base] if last else []) + pieces
        blocks = sum(piece.shape[0] for piece in pieces) // rows
        add_call = pl.pallas_call(
            functools.partial(add_pieces, dim, rows, factor if last else None),
            out_shape=small,
            in_specs=[VMEM] * len(operands),
            out_specs=VMEM,
            compiler_params=PARAMS,
            cost_estimate=pl.CostEstimate(
                flops=blocks * width * width * 400,
                bytes_accessed=4 * blocks * rows * width,
                transcendentals=2 * blocks * width * width,
            ),
        )
        total = add_call(*operands)
    return total


def solution(mesh):
    return jax.shard_map(
        on_device,
        mesh=mesh,
        in_specs=(P(None, ("gp", "blk")), P(None, ("gp", "blk")), P("gp"), P("gp")),
        out_specs=P(None, ("gp", "blk")),
        check_vma=False,
    )
```

```python
import functools
import math

import jax
import jax.numpy as jnp
from jax import lax
from jax.experimental import pallas as pl
from jax.experimental.pallas import tpu as pltpu
from jax.sharding import PartitionSpec as P


F32, BF16 = jnp.float32, jnp.bfloat16
LOG2E = math.log2(math.e)
SUBLANES = 8
VMEM = pl.BlockSpec(memory_space=pltpu.VMEM)
PARAMS = pltpu.CompilerParams(vmem_limit_bytes=8 * 2**20)


def split3(value):
    high = value.astype(BF16).astype(F32)
    rest = value - high
    middle = rest.astype(BF16).astype(F32)
    return high, middle, rest - middle


def norm_rows(value, norms_first):
    norm = jnp.sum(value * value, axis=0, keepdims=True)
    row = lax.broadcasted_iota(jnp.int32, (SUBLANES, value.shape[1]), 0)
    start = 0 if norms_first else 3
    rows = jnp.where(row < 6, 1.0, 0.0)
    for offset, addend in enumerate(split3(norm)):
        rows = jnp.where(row == start + offset, addend, rows)
    return rows


def stack(pieces):
    pieces = list(pieces)
    if sum(p.shape[0] for p in pieces) % (2 * SUBLANES):
        pieces.append(jnp.zeros_like(pieces[-1]))
    return jnp.concatenate(pieces, axis=0).astype(BF16)


def other_side(value):
    high, middle, low = split3(value)
    return stack([high, high, middle, middle, high, low, norm_rows(value, True)])


def own_side(value):
    high, middle, low = (-2.0 * part for part in split3(value))
    return stack([high, middle, high, middle, low, high, norm_rows(value, False)])


def third_kernel(value):
    value = jnp.maximum(value, 1e-30)
    third = value * lax.rsqrt(value)
    return (value + third + 1.0 / 3.0) * jnp.exp2(third * (-3.0 * LOG2E))


def block_sum(dim, block, scale, own):
    points, vectors = block[:dim] * scale, block[dim:]
    width = block.shape[1]
    other = other_side(points)
    vec_high = vectors.astype(BF16)
    vec = jnp.concatenate([vec_high, (vectors - vec_high.astype(F32)).astype(BF16)], axis=0)
    part = width // 2 if width % 256 == 0 else width
    both = 0.0
    for start in range(0, width, part):
        here = slice(start, start + part)
        value = lax.dot_general(
            other[:, here], own, (((0,), (0,)), ((), ())), preferred_element_type=F32
        )
        tile = third_kernel(value)
        high = tile.astype(BF16)
        low = (tile - high.astype(F32)).astype(BF16)
        both += jnp.dot(
            jnp.concatenate([vec[:, here]] * 2, axis=1),
            jnp.concatenate([high, low], axis=0),
            preferred_element_type=F32,
        )
    return both[: vectors.shape[0]] + both[vectors.shape[0] :]


def prepare(dim, own_ref, params_ref, scale_ref, side_ref, base_ref, sum_ref):
    here = lax.broadcasted_iota(jnp.int32, (dim, dim), 0) == lax.broadcasted_iota(
        jnp.int32, (dim, dim), 1
    )
    params = params_ref[...].reshape(1, dim + 1)
    inv = jnp.sum(jnp.where(here, params[:, :dim], 0.0), axis=1, keepdims=True)
    scale = jnp.broadcast_to(inv * (math.sqrt(5.0) / 3.0), scale_ref.shape)
    side = own_side(own_ref[:dim] * scale)
    scale_ref[...] = scale
    side_ref[...] = side
    base_ref[...] = own_ref[dim:] * params[:, dim:]
    sum_ref[...] = block_sum(dim, own_ref[...], scale, side)


def add_pieces(dim, rows, factor, scale_ref, side_ref, acc_ref, *rest):
    *rest, out_ref = rest
    base_ref = rest.pop(0) if factor else None
    scale, own = scale_ref[...], side_ref[...]
    total = acc_ref[...]
    for piece_ref in rest:
        count = piece_ref.shape[0] // rows
        group = count if count <= 8 else math.gcd(count, 8)

        def step(index, total, piece_ref=piece_ref, group=group):
            for k in range(group):
                start = pl.multiple_of((index * group + k) * rows, rows)
                total = total + block_sum(dim, piece_ref[pl.ds(start, rows)], scale, own)
            return total

        if count == group:
            total = step(0, total)
        else:
            total = lax.fori_loop(0, count // group, step, total)
    out_ref[...] = base_ref[...] + total * factor if factor else total


def on_device(points, vectors, inv_length, noise):
    count = lax.axis_size("blk")
    dim, width = points.shape
    rhs = vectors.shape[0]
    rows = dim + rhs
    small = jax.ShapeDtypeStruct((rhs, width), F32)
    own = lax.optimization_barrier(jnp.concatenate([points, vectors], axis=0))
    params = lax.optimization_barrier(jnp.concatenate([inv_length, noise]))

    def swap(value, mask):
        return lax.ppermute(value, "blk", [(i, i ^ mask) for i in range(count)])

    levels = count.bit_length() - 1
    if count != 1 << levels or levels < 3:
        turns = [[(i, (i + k) % count) for i in range(count)] for k in range(1, count)]
        groups = [[lax.ppermute(own, "blk", pairs) for pairs in turns]]
    else:
        held, others = own, []
        for bit in range(levels - 1, 2, -1):
            others.append(swap(held, 1 << bit | 1))
            held = jnp.concatenate([held, others[-1]], axis=0)
        newest = swap(held, 3)
        early = swap(held, 5)
        late = swap(newest, 5)
        near_held = swap(held, 1)
        near = swap(jnp.concatenate([newest, early], axis=0), 1)
        late_core = swap(late, 1)
        groups = [others + [newest, early, near_held], [near, late], [late_core]]

    side_rows = -(-(6 * dim + SUBLANES) // (2 * SUBLANES)) * 2 * SUBLANES
    prepare_call = pl.pallas_call(
        functools.partial(prepare, dim),
        out_shape=[
            jax.ShapeDtypeStruct((dim, width), F32),
            jax.ShapeDtypeStruct((side_rows, width), BF16),
            small,
            small,
        ],
        in_specs=[VMEM] * 2,
        out_specs=[VMEM] * 4,
        name="prepare",
        compiler_params=PARAMS,
        cost_estimate=pl.CostEstimate(flops=100000, bytes_accessed=4 * rows * width, transcendentals=0),
    )
    scale, side, base, total = prepare_call(own, params)

    factor = 3.0 / math.sqrt(width * count)
    for index, pieces in enumerate(groups):
        last = index == len(groups) - 1
        operands = [scale, side, total] + ([base] if last else []) + pieces
        blocks = sum(piece.shape[0] for piece in pieces) // rows
        add_call = pl.pallas_call(
            functools.partial(add_pieces, dim, rows, factor if last else None),
            out_shape=small,
            in_specs=[VMEM] * len(operands),
            out_specs=VMEM,
            compiler_params=PARAMS,
            cost_estimate=pl.CostEstimate(
                flops=blocks * width * width * 400,
                bytes_accessed=4 * blocks * rows * width,
                transcendentals=2 * blocks * width * width,
            ),
        )
        total = add_call(*operands)
    return total


def solution(mesh):
    return jax.shard_map(
        on_device,
        mesh=mesh,
        in_specs=(P(None, ("gp", "blk")), P(None, ("gp", "blk")), P("gp"), P("gp")),
        out_specs=P(None, ("gp", "blk")),
        check_vma=False,
    )
```

```python
import functools
import math

import jax
import jax.numpy as jnp
from jax import lax
from jax.experimental import pallas as pl
from jax.experimental.pallas import tpu as pltpu
from jax.sharding import PartitionSpec as P


F32, BF16 = jnp.float32, jnp.bfloat16
LOG2E = math.log2(math.e)
SUBLANES = 8
VMEM = pl.BlockSpec(memory_space=pltpu.VMEM)
PARAMS = pltpu.CompilerParams(vmem_limit_bytes=8 * 2**20)


def split3(value):
    high = value.astype(BF16).astype(F32)
    rest = value - high
    middle = rest.astype(BF16).astype(F32)
    return high, middle, rest - middle


def norm_rows(value, norms_first):
    norm = jnp.sum(value * value, axis=0, keepdims=True)
    row = lax.broadcasted_iota(jnp.int32, (SUBLANES, value.shape[1]), 0)
    start = 0 if norms_first else 3
    rows = jnp.where(row < 6, 1.0, 0.0)
    for offset, addend in enumerate(split3(norm)):
        rows = jnp.where(row == start + offset, addend, rows)
    return rows


def stack(pieces):
    pieces = list(pieces)
    if sum(p.shape[0] for p in pieces) % (2 * SUBLANES):
        pieces.append(jnp.zeros_like(pieces[-1]))
    return jnp.concatenate(pieces, axis=0).astype(BF16)


def other_side(value):
    high, middle, low = split3(value)
    return stack([high, high, middle, middle, high, low, norm_rows(value, True)])


def own_side(value):
    high, middle, low = (-2.0 * part for part in split3(value))
    return stack([high, middle, high, middle, low, high, norm_rows(value, False)])


def third_kernel(value):
    value = jnp.maximum(value, 1e-30)
    third = value * lax.rsqrt(value)
    return (value + third + 1.0 / 3.0) * jnp.exp2(third * (-3.0 * LOG2E))


def block_sum(dim, block, scale, own):
    points, vectors = block[:dim] * scale, block[dim:]
    width = block.shape[1]
    other = other_side(points)
    vec_high = vectors.astype(BF16)
    vec = jnp.concatenate([vec_high, (vectors - vec_high.astype(F32)).astype(BF16)], axis=0)
    part = width // 2 if width % 256 == 0 else width
    both = 0.0
    for start in range(0, width, part):
        here = slice(start, start + part)
        value = lax.dot_general(
            other[:, here], own, (((0,), (0,)), ((), ())), preferred_element_type=F32
        )
        tile = third_kernel(value)
        high = tile.astype(BF16)
        low = (tile - high.astype(F32)).astype(BF16)
        both += jnp.dot(
            jnp.concatenate([vec[:, here]] * 2, axis=1),
            jnp.concatenate([high, low], axis=0),
            preferred_element_type=F32,
        )
    return both[: vectors.shape[0]] + both[vectors.shape[0] :]


def prepare(dim, own_ref, params_ref, scale_ref, side_ref, base_ref, sum_ref):
    here = lax.broadcasted_iota(jnp.int32, (dim, dim), 0) == lax.broadcasted_iota(
        jnp.int32, (dim, dim), 1
    )
    params = params_ref[...].reshape(1, dim + 1)
    inv = jnp.sum(jnp.where(here, params[:, :dim], 0.0), axis=1, keepdims=True)
    scale = jnp.broadcast_to(inv * (math.sqrt(5.0) / 3.0), scale_ref.shape)
    side = own_side(own_ref[:dim] * scale)
    scale_ref[...] = scale
    side_ref[...] = side
    base_ref[...] = own_ref[dim:] * params[:, dim:]
    sum_ref[...] = block_sum(dim, own_ref[...], scale, side)


def add_pieces(dim, rows, factor, scale_ref, side_ref, acc_ref, *rest):
    *rest, out_ref = rest
    base_ref = rest.pop(0) if factor else None
    scale, own = scale_ref[...], side_ref[...]
    total = acc_ref[...]
    for piece_ref in rest:
        count = piece_ref.shape[0] // rows
        group = count if count <= 8 else math.gcd(count, 8)

        def step(index, total, piece_ref=piece_ref, group=group):
            for k in range(group):
                start = pl.multiple_of((index * group + k) * rows, rows)
                total = total + block_sum(dim, piece_ref[pl.ds(start, rows)], scale, own)
            return total

        if count == group:
            total = step(0, total)
        else:
            total = lax.fori_loop(0, count // group, step, total)
    out_ref[...] = base_ref[...] + total * factor if factor else total


def on_device(points, vectors, inv_length, noise):
    count = lax.axis_size("blk")
    dim, width = points.shape
    rhs = vectors.shape[0]
    rows = dim + rhs
    small = jax.ShapeDtypeStruct((rhs, width), F32)
    own = lax.optimization_barrier(jnp.concatenate([points, vectors], axis=0))
    params = lax.optimization_barrier(jnp.concatenate([inv_length, noise]))

    def swap(value, mask):
        return lax.ppermute(value, "blk", [(i, i ^ mask) for i in range(count)])

    levels = count.bit_length() - 1
    if count != 1 << levels or levels < 3:
        turns = [[(i, (i + k) % count) for i in range(count)] for k in range(1, count)]
        groups = [[lax.ppermute(own, "blk", pairs) for pairs in turns]]
    else:
        held, others = own, []
        for _ in range(levels - 1, 2, -1):
            others.append(swap(held, 9))
            held = jnp.concatenate([held, others[-1]], axis=0)
        newest = swap(held, 5)
        early = swap(held, 3)
        late = swap(newest, 3)
        near_held = swap(held, 1)
        near = swap(jnp.concatenate([newest, early], axis=0), 1)
        late_core = swap(late, 1)
        groups = [others + [newest, early, near_held], [near, late], [late_core]]

    side_rows = -(-(6 * dim + SUBLANES) // (2 * SUBLANES)) * 2 * SUBLANES
    prepare_call = pl.pallas_call(
        functools.partial(prepare, dim),
        out_shape=[
            jax.ShapeDtypeStruct((dim, width), F32),
            jax.ShapeDtypeStruct((side_rows, width), BF16),
            small,
            small,
        ],
        in_specs=[VMEM] * 2,
        out_specs=[VMEM] * 4,
        name="prepare",
        compiler_params=PARAMS,
        cost_estimate=pl.CostEstimate(flops=100000, bytes_accessed=4 * rows * width, transcendentals=0),
    )
    scale, side, base, total = prepare_call(own, params)

    factor = 3.0 / math.sqrt(width * count)
    for index, pieces in enumerate(groups):
        last = index == len(groups) - 1
        operands = [scale, side, total] + ([base] if last else []) + pieces
        blocks = sum(piece.shape[0] for piece in pieces) // rows
        add_call = pl.pallas_call(
            functools.partial(add_pieces, dim, rows, factor if last else None),
            out_shape=small,
            in_specs=[VMEM] * len(operands),
            out_specs=VMEM,
            compiler_params=PARAMS,
            cost_estimate=pl.CostEstimate(
                flops=blocks * width * width * 400,
                bytes_accessed=4 * blocks * rows * width,
                transcendentals=2 * blocks * width * width,
            ),
        )
        total = add_call(*operands)
    return total


def solution(mesh):
    return jax.shard_map(
        on_device,
        mesh=mesh,
        in_specs=(P(None, ("gp", "blk")), P(None, ("gp", "blk")), P("gp"), P("gp")),
        out_specs=P(None, ("gp", "blk")),
        check_vma=False,
    )
```
